32 devices in a mesh: aa: 8 (over z, y), ba: 4 (over x, core).
Axes of the slice: x: 2, y: 2, z: 4, core: 2. Of those that a mesh axis runs over, the one named last changes fastest.
Arguments:
- tokens: bfloat16 [4096, 8192], P('aa', 'ba'), may hold values from -6 to 6
- request_adapter_index: int32 [4096, 1], P('aa'), may hold values from 0 to 127; in each aligned block of 512 rows (0 to 511, 512 to 1023, ...) at most 8 rows name the same one
- key_weight: bfloat16 [8192, 1024], P('ba'), may hold values from -0.0625 to 0.0625
- value_weight: bfloat16 [8192, 1024], P('ba'), may hold values from -0.0625 to 0.0625
- adapter_down_weight: bfloat16 [128, 32, 8192], P('aa', None, 'ba'), may hold values from -0.0625 to 0.0625
- adapter_up_weight: bfloat16 [128, 2, 16, 1024], P('aa'), may hold values from -1.5 to 1.5
Outputs:
- keys_out: bfloat16 [4096, 1024], P('aa', 'ba')
- values_out: bfloat16 [4096, 1024], P('aa', 'ba')
The draws below stay inside these ranges and needn't reach their ends.
Inputs may be any that keep to these rules, and one draw needn't show every extreme that they name: `request_adapter_index`: among the 512 rows of one device no adapter is named more than 8 times, a bound that some block reaches.
All inputs are finite; a program needn't handle non-finite values.
Results may differ from the reference program's by a relative error of at most 0.001.
Values may be sent and summed in bfloat16 or wider, within the bound.
A program may use at most 128 MiB of HBM per device.

```python
import math
import jax
import jax.numpy as jnp
import numpy as np
from jax import lax

MODEL_WIDTH = 8192
KEY_VALUE_WIDTH = 1024
ADAPTER_RANK = 16
ADAPTER_COUNT = 128
TOK_DEV = 512
TOKENS = 4096
ACAP = 8


def block_scale(stream_key, dims, split, least, high):
    gain, own = 1.0, jax.random.fold_in(stream_key, 6)
    for axis_at, blocks in split:
        heights = jnp.exp(jax.random.uniform(jax.random.fold_in(own, axis_at), (blocks,), jnp.float32, least / len(split), high / len(split)))
        gain = gain * jnp.repeat(heights, dims[axis_at] // blocks).reshape([-1 if axis == axis_at else 1 for axis in range(len(dims))])
    return gain


def shared_out(stream_key, own, number, rows, count, top, limit, lean):
    sequence = jax.random.permutation(stream_key, count)
    heavy_load, usual = portions_of(count, rows * top, limit, lean, True), portions_of(count, rows * top, limit, lean, False)
    places = jnp.arange(count)

    def named(tallies, offset_by):
        used = int((tallies > 0).sum())
        fixed = max(1, used // 4)
        shifted = fixed + (places - fixed + offset_by * (used - fixed)) % max(1, count - fixed)
        return jnp.zeros((count,), jnp.int32).at[sequence[jnp.where(places < fixed, places, shifted)]].set(jnp.asarray(tallies, jnp.int32))

    tallies = jnp.where(number % 4 == 0, named(heavy_load, number // 4), named(usual, number - number // 4 - 1))
    mixed = jax.random.permutation(jax.random.fold_in(own, 3), count)
    giver, sink = mixed[0:count // 2 * 2:2], mixed[1:count // 2 * 2:2]
    room = jnp.minimum(tallies[giver] - 1, limit - tallies[sink]) // 2
    room = jnp.where((giver == sequence[0]) | (sink == sequence[0]) | (tallies[sink] == 0), 0, jnp.maximum(room, 0))
    shifted = jax.random.randint(jax.random.fold_in(own, 4), (count // 2,), 0, 1 << 20) % (room + 1)
    tallies = tallies.at[giver].add(-shifted).at[sink].add(shifted)
    labels = jnp.searchsorted(jnp.cumsum(tallies), jnp.arange(rows * top), side="right").astype(jnp.int32)
    listing = labels.reshape(top, rows).T
    listing = listing[jax.random.permutation(jax.random.fold_in(own, 1), rows)]
    offset_by = jax.random.randint(jax.random.fold_in(own, 2), (rows, 1), 0, top)
    return jnp.take_along_axis(listing, (jnp.arange(top)[None, :] + offset_by) % top, axis=1)


def portions_of(number_of, total, reach, slope, full):
    portions = [(1 << 20) // math.isqrt(standing ** slope) + 1 for standing in range(1, number_of + 1)]
    largest = reach if full else min(reach, max(-(-total // number_of), total * portions[0] // sum(portions)))
    least = 1 if total - largest >= number_of - 1 else 0
    counts, rest = [largest] + [least] * (number_of - 1), total - largest - least * (number_of - 1)
    while rest > 0:
        movable = [i for i in range(1, number_of) if counts[i] < largest] or [i for i in range(1, number_of) if counts[i] < reach]
        whole, remaining = sum([portions[i] for i in movable]), rest
        for i in movable:
            addition = min(reach - counts[i], max(1, remaining * portions[i] // whole), rest)
            counts[i] = counts[i] + addition
            rest = rest - addition
    return np.array(counts)


def noise(own_key, extent, deviation, limit, cuts=(), kind=jnp.bfloat16):
    entries = jax.random.normal(own_key, extent, jnp.float32) * deviation
    if len(cuts) > 0:
        entries = block_scale(own_key, extent, cuts, -0.22, 0.18) * entries
    return jnp.clip(entries, min=-limit, max=limit).astype(kind)


def setup_inputs(seed: int = 0) -> dict:
    splits = jax.random.split(jax.random.key(seed), 7)
    tokens = noise(splits[0], (TOKENS, MODEL_WIDTH), 1.0, 6.0, ((0, 8), (1, 4)))
    request_adapter_index_keys = jax.random.split(jax.random.fold_in(splits[1], 1), TOKENS // TOK_DEV)
    request_adapter_index_turns = jax.random.permutation(jax.random.fold_in(splits[1], 3), TOKENS // TOK_DEV)
    request_adapter_index = jax.vmap(lambda own, number: shared_out(jax.random.fold_in(splits[1], 2), own, number, TOK_DEV, ADAPTER_COUNT, 1, ACAP, 2))(request_adapter_index_keys, request_adapter_index_turns).reshape((TOKENS, 1))
    key_weight = noise(splits[2], (MODEL_WIDTH, KEY_VALUE_WIDTH), MODEL_WIDTH ** -0.5, 0.0625, ((0, 4),))
    value_weight = noise(splits[3], (MODEL_WIDTH, KEY_VALUE_WIDTH), MODEL_WIDTH ** -0.5, 0.0625, ((0, 4),))
    adapter_down_weight = noise(splits[4], (ADAPTER_COUNT, 2 * ADAPTER_RANK, MODEL_WIDTH), MODEL_WIDTH ** -0.5, 0.0625, ((0, 8), (2, 4)))
    adapter_up_weight = noise(splits[5], (ADAPTER_COUNT, 2, ADAPTER_RANK, KEY_VALUE_WIDTH), ADAPTER_RANK ** -0.5, 1.5, ((0, 8),))
    return {"tokens": tokens, "request_adapter_index": request_adapter_index, "key_weight": key_weight, "value_weight": value_weight, "adapter_down_weight": adapter_down_weight, "adapter_up_weight": adapter_up_weight}


def reference(tokens, request_adapter_index, key_weight, value_weight, adapter_down_weight, adapter_up_weight):
    base_key = jnp.dot(tokens, key_weight, preferred_element_type=jnp.float32)
    base_value = jnp.dot(tokens, value_weight, preferred_element_type=jnp.float32)
    height = math.gcd(TOKENS, 64)
    token_blocks = tokens.reshape(TOKENS // height, height, MODEL_WIDTH)
    adapter_blocks = request_adapter_index.reshape(TOKENS // height, height)

    def one_block(pair):
        rows, selected_adapter = pair
        down_weight_rows = adapter_down_weight[selected_adapter].astype(jnp.float32)
        up_weight_rows = adapter_up_weight[selected_adapter].astype(jnp.float32)
        rank_sum = jnp.einsum("td,tjd->tj", rows.astype(jnp.float32), down_weight_rows, precision=lax.Precision.HIGHEST)
        key_change = jnp.einsum("tr,trc->tc", rank_sum[:, :ADAPTER_RANK], up_weight_rows[:, 0], precision=lax.Precision.HIGHEST)
        value_change = jnp.einsum("tr,trc->tc", rank_sum[:, ADAPTER_RANK:], up_weight_rows[:, 1], precision=lax.Precision.HIGHEST)
        return key_change, value_change

    key_change, value_change = lax.map(one_block, (token_blocks, adapter_blocks))
    keys_out = (base_key + key_change.reshape(TOKENS, KEY_VALUE_WIDTH)).astype(jnp.bfloat16)
    values_out = (base_value + value_change.reshape(TOKENS, KEY_VALUE_WIDTH)).astype(jnp.bfloat16)
    return keys_out, values_out
```

```python
import functools

import jax
import jax.numpy as jnp
from jax import lax
from jax.experimental import pallas as pl
from jax.experimental.pallas import tpu as pltpu
from jax.sharding import PartitionSpec as P

MESH = pl.DeviceIdType.MESH
LANES = 128
BF16 = jnp.bfloat16
F32 = jnp.float32


def split_two(x):
    hi = x.astype(BF16)
    return hi, (x - hi.astype(F32)).astype(BF16)


def kernel(
    n, m, cap, resident, twice_rank,
    idx_col, idx_row, tok_hbm, kw_hbm, vw_hbm, down_hbm, up_hbm,
    keys_out, values_out,
    tok, kw, vw, down, up_all, outgoing, recv, rs_send, rs_recv,
    rank_part, rank_in, ret_send, ret_recv,
    load_sem, up_send_sem, up_recv_sem, d_send_sem, d_recv_sem,
    rs_send_sem, rs_recv_sem, p_send_sem, p_recv_sem, r_send_sem, r_recv_sem,
):
    me = lax.axis_index("aa")
    mb = lax.axis_index("ba")
    rows = tok.shape[0]
    kv = keys_out.shape[1]
    groups = LANES // twice_rank
    quads = resident // groups
    stride = cap * quads
    chunk = resident * cap
    rank = twice_rank // 2

    loads = [
        pltpu.make_async_copy(tok_hbm, tok, load_sem.at[0]),
        pltpu.make_async_copy(
            up_hbm.at[:, pl.ds(pl.multiple_of(mb * kv, LANES), kv)], up_all.at[me], load_sem.at[1]
        ),
        pltpu.make_async_copy(kw_hbm, kw, load_sem.at[2]),
        pltpu.make_async_copy(vw_hbm, vw, load_sem.at[3]),
        pltpu.make_async_copy(down_hbm, down, load_sem.at[4]),
    ]
    for c in loads:
        c.start()

    barrier = pltpu.get_barrier_semaphore()

    def greet_aa(i, _):
        pl.semaphore_signal(barrier, inc=1, device_id={"aa": lax.rem(me + i, n)}, device_id_type=MESH)
        return 0

    def greet_ba(i, _):
        pl.semaphore_signal(barrier, inc=1, device_id={"ba": lax.rem(mb + i, m)}, device_id_type=MESH)
        return 0

    lax.fori_loop(1, n, greet_aa, 0)
    lax.fori_loop(1, m, greet_ba, 0)

    def slot(a, earlier):
        local = lax.rem(a, resident)
        return (a // resident) * chunk + lax.rem(local, groups) * stride + earlier * quads + local // groups

    col, row = idx_col[...], idx_row[...]
    same = col == row
    down_pos = lax.broadcasted_iota(jnp.int32, (rows, rows), 0)
    lane_pos = lax.broadcasted_iota(jnp.int32, (rows, rows), 1)
    slot_col = slot(col, jnp.sum(jnp.where(same & (lane_pos < down_pos), 1, 0), axis=1, keepdims=True))
    slot_row = slot(row, jnp.sum(jnp.where(same & (down_pos < lane_pos), 1, 0), axis=0, keepdims=True))

    def offset(i):
        j = i - 1
        h = (j + 1) // 2
        return jnp.where(i == 0, 0, n // 2 + (1 - 2 * lax.rem(j + 2, 2)) * h)

    def peer(i):
        return lax.rem(me + offset(i), n)

    def dispatch(i):
        return pltpu.make_async_remote_copy(
            src_ref=outgoing.at[i], dst_ref=recv.at[i],
            send_sem=d_send_sem.at[i], recv_sem=d_recv_sem.at[i],
            device_id={"aa": peer(i)}, device_id_type=MESH,
        )

    def fill(i):
        wanted = lax.broadcasted_iota(jnp.int32, (chunk, rows), 0) + peer(i) * chunk
        pick = jnp.where(wanted == slot_row, 1.0, 0.0).astype(BF16)
        return jnp.dot(pick, tok[...], preferred_element_type=F32).astype(BF16)

    bits = []
    bit = n // 2
    while bit:
        bits.append(bit)
        bit //= 2

    def flip(x, b):
        return x + b - 2 * b * lax.rem(x // b, 2)

    up_copies = []
    held = [()]
    number = 0
    for b in bits:
        stage = []
        for path in held:
            block = me
            for q in path:
                block = flip(block, q)
            stage.append((block, flip(me, b), number))
            number += 1
        up_copies.append(stage)
        held = held + [path + (b,) for path in held]

    def up_copy(block, partner, at):
        return pltpu.make_async_remote_copy(
            src_ref=up_all.at[block], dst_ref=up_all.at[block],
            send_sem=up_send_sem.at[at], recv_sem=up_recv_sem.at[at],
            device_id={"aa": partner}, device_id_type=MESH,
        )

    pl.semaphore_wait(barrier, n + m - 2)
    loads[1].wait()
    loads[0].wait()

    def send_one(i, _):
        outgoing[i] = fill(i)
        dispatch(i).start()
        return 0

    def up_stage(at):
        if at > 0:
            for entry in up_copies[at - 1]:
                up_copy(*entry).wait_recv()
        if at < len(up_copies):
            for entry in up_copies[at]:
                up_copy(*entry).start()

    lax.fori_loop(1, 2, send_one, 0)
    up_stage(0)
    lax.fori_loop(2, n, send_one, 0)
    recv[0] = fill(0)

    loads[2].wait()
    loads[3].wait()

    def rs_copy(b):
        return pltpu.make_async_remote_copy(
            src_ref=rs_send.at[b], dst_ref=rs_recv.at[b],
            send_sem=rs_send_sem.at[b], recv_sem=rs_recv_sem.at[b],
            device_id={"ba": lax.rem(mb + b + 1, m)}, device_id_type=MESH,
        )

    def base(b, _):
        cols = pl.ds(pl.multiple_of(lax.rem(mb + b + 1, m) * kv, LANES), kv)
        rs_send[b, :, :kv] = jnp.dot(tok[...], kw[:, cols], preferred_element_type=F32)
        rs_send[b, :, kv:] = jnp.dot(tok[...], vw[:, cols], preferred_element_type=F32)

        @pl.when(b < m - 1)
        def _():
            rs_copy(b).start()

        return 0

    lax.fori_loop(0, m, base, 0)
    for at in range(1, len(up_copies) + 1):
        up_stage(at)
    loads[4].wait()
    acc = rs_send.at[m - 1]

    def add_part(b, _):
        rs_copy(b).wait_recv()
        acc[...] += rs_recv[b]
        return 0

    lax.fori_loop(0, m - 1, add_part, 0)

    width = resident * twice_rank
    slot_of_row = lax.broadcasted_iota(jnp.int32, (chunk, width), 0)
    column = lax.broadcasted_iota(jnp.int32, (chunk, width), 1)
    adapter_of_row = lax.rem(slot_of_row, quads) * groups + slot_of_row // stride
    own = adapter_of_row == column // twice_rank
    for_key = lax.rem(column, twice_rank) < rank

    def part_copy(b, i):
        return pltpu.make_async_remote_copy(
            src_ref=rank_part.at[i], dst_ref=rank_in.at[b, i],
            send_sem=p_send_sem.at[b, i], recv_sem=p_recv_sem.at[b, i],
            device_id={"ba": lax.rem(mb + b + 1, m)}, device_id_type=MESH,
        )

    def ret_copy(i):
        return pltpu.make_async_remote_copy(
            src_ref=ret_send.at[i], dst_ref=ret_recv.at[i],
            send_sem=r_send_sem.at[i], recv_sem=r_recv_sem.at[i],
            device_id={"aa": lax.rem(me - offset(i) + n, n)}, device_id_type=MESH,
        )

    def partial(i):
        @pl.when(i > 0)
        def _():
            dispatch(i).wait_recv()

        wide = lax.dot_general(
            recv[i], down[...], (((1,), (1,)), ((), ())), preferred_element_type=F32
        )
        wide = jnp.where(own, wide, 0.0)
        total = wide[:, :LANES]
        for q in range(1, width // LANES):
            total = total + wide[:, q * LANES:(q + 1) * LANES]
        packed = total[:stride]
        for g in range(1, groups):
            packed = packed + total[g * stride:(g + 1) * stride]
        rank_part[i] = packed
        for b in range(m - 1):
            part_copy(b, i).start()

    def finish(i):
        total = rank_part[i]
        for b in range(m - 1):
            part_copy(b, i).wait_recv()
            total = total + rank_in[b, i]

        @pl.when(i == 0)
        def _():
            ret_recv[i] = total

        @pl.when(i > 0)
        def _():
            ret_send[i] = total
            ret_copy(i).start()

    def final(i):
        @pl.when(i > 0)
        def _():
            ret_copy(i).wait_recv()

        tall = jnp.concatenate([ret_recv[i]] * groups, axis=0)
        spread = jnp.where(own, jnp.concatenate([tall] * (width // LANES), axis=1), 0.0)
        key_hi, key_lo = split_two(jnp.where(for_key, spread, 0.0))
        value_hi, value_lo = split_two(jnp.where(for_key, 0.0, spread))
        bank = peer(i)
        up = up_all[bank]
        pieces = jnp.concatenate([key_hi, key_lo, value_hi, value_lo], axis=0)
        out = jnp.dot(pieces, up, preferred_element_type=F32)
        change = jnp.concatenate(
            [out[:chunk] + out[chunk:2 * chunk], out[2 * chunk:3 * chunk] + out[3 * chunk:]], axis=1
        )
        hi, lo = split_two(change)
        place = lax.broadcasted_iota(jnp.int32, (rows, chunk), 1) + bank * chunk
        pick = jnp.where(place == slot_col, 1.0, 0.0).astype(BF16)
        acc[...] += jnp.dot(pick, hi, preferred_element_type=F32) + jnp.dot(
            pick, lo, preferred_element_type=F32
        )

    def step(t, _):
        @pl.when(t < n)
        def _():
            partial(t)

        @pl.when((t >= 1) & (t < n + 1))
        def _():
            finish(t - 1)

        @pl.when(t >= 2)
        def _():
            final(t - 2)

        return 0

    lax.fori_loop(0, n + 2, step, 0)
    keys_out[...] = acc[:, :kv].astype(keys_out.dtype)
    values_out[...] = acc[:, kv:].astype(values_out.dtype)

    for stage in up_copies:
        for entry in stage:
            up_copy(*entry).wait_send()

    def drain(i, _):
        dispatch(i).wait_send()
        ret_copy(i).wait_send()
        return 0

    lax.fori_loop(1, n, drain, 0)

    def drain_parts(i, _):
        for b in range(m - 1):
            part_copy(b, i).wait_send()
        return 0

    lax.fori_loop(0, n, drain_parts, 0)
    for b in range(m - 1):
        rs_copy(b).wait_send()


def on_device(n, m, tokens, request_adapter_index, key_weight, value_weight, down_weight, up_weight):
    rows, width = tokens.shape
    resident, twice_rank, _ = down_weight.shape
    kv_width = key_weight.shape[1]
    kv = kv_width // m
    cap = max(2, 2 * rows // (resident * n))
    chunk = resident * cap
    packed = chunk * twice_rank // LANES
    flat = resident * twice_rank
    dma = pltpu.SemaphoreType.DMA
    return pl.pallas_call(
        functools.partial(kernel, n, m, cap, resident, twice_rank),
        out_shape=[jax.ShapeDtypeStruct((rows, kv), BF16)] * 2,
        in_specs=[pl.BlockSpec(memory_space=pltpu.VMEM)] * 2 + [pl.BlockSpec(memory_space=pl.ANY)] * 5,
        out_specs=[pl.BlockSpec(memory_space=pltpu.VMEM)] * 2,
        scratch_shapes=[
            pltpu.VMEM((rows, width), BF16),
            pltpu.VMEM((width, kv_width), BF16),
            pltpu.VMEM((width, kv_width), BF16),
            pltpu.VMEM((flat, width), BF16),
            pltpu.VMEM((n, flat, kv), BF16),
            pltpu.VMEM((n, chunk, width), BF16),
            pltpu.VMEM((n, chunk, width), BF16),
            pltpu.VMEM((m, rows, 2 * kv), F32),
            pltpu.VMEM((m - 1, rows, 2 * kv), F32),
            pltpu.VMEM((n, packed, LANES), F32),
            pltpu.VMEM((m - 1, n, packed, LANES), F32),
            pltpu.VMEM((n, packed, LANES), F32),
            pltpu.VMEM((n, packed, LANES), F32),
            dma((5,)),
            dma((n,)), dma((n,)), dma((n,)), dma((n,)),
            dma((m,)), dma((m,)),
            dma((m - 1, n)), dma((m - 1, n)),
            dma((n,)), dma((n,)),
        ],
        compiler_params=pltpu.CompilerParams(
            collective_id=0, has_side_effects=True, vmem_limit_bytes=56 * 1024 * 1024
        ),
    )(
        request_adapter_index,
        request_adapter_index.reshape(1, rows),
        tokens,
        key_weight,
        value_weight,
        down_weight.reshape(flat, width),
        up_weight.reshape(flat, kv_width),
    )


def solution(mesh):
    return jax.shard_map(
        functools.partial(on_device, mesh.shape["aa"], mesh.shape["ba"]),
        mesh=mesh,
        in_specs=(
            P("aa", "ba"),
            P("aa", None),
            P("ba", None),
            P("ba", None),
            P("aa", None, "ba"),
            P("aa", None, None, None),
        ),
        out_specs=(P("aa", "ba"), P("aa", "ba")),
        check_vma=False,
    )
```

```python
import functools

import jax
import jax.numpy as jnp
from jax import lax
from jax.experimental import pallas as pl
from jax.experimental.pallas import tpu as pltpu
from jax.sharding import PartitionSpec as P

MESH = pl.DeviceIdType.MESH
LANES = 128
BF16 = jnp.bfloat16
F32 = jnp.float32


def split_two(x):
    hi = x.astype(BF16)
    return hi, (x - hi.astype(F32)).astype(BF16)


def kernel(
    n, m, cap, resident, twice_rank,
    idx_row, tok_hbm, kw_hbm, vw_hbm, down_hbm, up_hbm,
    acc,
    tok, kw, vw, down, up_all, outgoing, recv, rs_send, rs_recv,
    rank_part, rank_in, ret_send, ret_recv,
    load_sem, up_send_sem, up_recv_sem, d_send_sem, d_recv_sem,
    rs_send_sem, rs_recv_sem, p_send_sem, p_recv_sem, r_send_sem, r_recv_sem,
):
    me = lax.axis_index("aa")
    mb = lax.axis_index("ba")
    rows = tok.shape[0]
    kv = acc.shape[1] // 2
    groups = LANES // twice_rank
    quads = resident // groups
    stride = cap * quads
    chunk = resident * cap
    rank = twice_rank // 2

    loads = [
        pltpu.make_async_copy(tok_hbm, tok, load_sem.at[0]),
        pltpu.make_async_copy(
            up_hbm.at[:, pl.ds(pl.multiple_of(mb * kv, LANES), kv)], up_all.at[me], load_sem.at[1]
        ),
        pltpu.make_async_copy(kw_hbm, kw, load_sem.at[2]),
        pltpu.make_async_copy(vw_hbm, vw, load_sem.at[3]),
        pltpu.make_async_copy(down_hbm, down, load_sem.at[4]),
    ]
    for c in loads:
        c.start()

    barrier = pltpu.get_barrier_semaphore()

    def greet_aa(i, _):
        pl.semaphore_signal(barrier, inc=1, device_id={"aa": lax.rem(me + i, n)}, device_id_type=MESH)
        return 0

    def greet_ba(i, _):
        pl.semaphore_signal(barrier, inc=1, device_id={"ba": lax.rem(mb + i, m)}, device_id_type=MESH)
        return 0

    lax.fori_loop(1, n, greet_aa, 0)
    lax.fori_loop(1, m, greet_ba, 0)

    def slot(a, earlier):
        local = lax.rem(a, resident)
        return (a // resident) * chunk + lax.rem(local, groups) * stride + earlier * quads + local // groups

    row = idx_row[...]
    down_pos = lax.broadcasted_iota(jnp.int32, (rows, rows), 0)
    lane_pos = lax.broadcasted_iota(jnp.int32, (rows, rows), 1)
    col = jnp.sum(jnp.where(down_pos == lane_pos, row, 0), axis=1, keepdims=True)
    same = col == row
    slot_col = slot(col, jnp.sum(jnp.where(same & (lane_pos < down_pos), 1, 0), axis=1, keepdims=True))
    slot_row = slot(row, jnp.sum(jnp.where(same & (down_pos < lane_pos), 1, 0), axis=0, keepdims=True))

    def flip(x, b):
        return x + b - 2 * b * lax.rem(x // b, 2)

    bits = []
    bit = n // 2
    while bit:
        bits.append(bit)
        bit //= 2

    far = list(range(n // 2, n))
    near = list(range(n // 4, n // 2))
    order = [0]
    while far:
        if near:
            order.append(near.pop(0))
        order.append(far.pop(0))
    order += near + [d for d in range(n // 4 - 1, 0, -1)]

    def peer(i):
        mask = sum([jnp.where(i == at, order[at], 0) for at in range(1, n)], jnp.int32(0))
        other = me
        for b in bits:
            other = jnp.where(lax.rem(mask // b, 2) == 1, flip(other, b), other)
        return other

    def dispatch(i):
        return pltpu.make_async_remote_copy(
            src_ref=outgoing.at[i], dst_ref=recv.at[i],
            send_sem=d_send_sem.at[i], recv_sem=d_recv_sem.at[i],
            device_id={"aa": peer(i)}, device_id_type=MESH,
        )

    def fill(i):
        wanted = lax.broadcasted_iota(jnp.int32, (chunk, rows), 0) + peer(i) * chunk
        pick = jnp.where(wanted == slot_row, 1.0, 0.0).astype(BF16)
        return jnp.dot(pick, tok[...], preferred_element_type=F32).astype(BF16)

    up_copies = []
    held = [()]
    number = 0
    for b in bits:
        stage = []
        for path in held:
            block = me
            for q in path:
                block = flip(block, q)
            stage.append((block, flip(me, b), number))
            number += 1
        up_copies.append(stage)
        held = held + [path + (b,) for path in held]

    def up_copy(block, partner, at):
        return pltpu.make_async_remote_copy(
            src_ref=up_all.at[block], dst_ref=up_all.at[block],
            send_sem=up_send_sem.at[at], recv_sem=up_recv_sem.at[at],
            device_id={"aa": partner}, device_id_type=MESH,
        )

    pl.semaphore_wait(barrier, n + m - 2)
    loads[1].wait()
    loads[0].wait()

    def send_one(i, _):
        outgoing[i] = fill(i)
        dispatch(i).start()
        return 0

    def up_stage(at):
        if at > 0:
            for entry in up_copies[at - 1]:
                up_copy(*entry).wait_recv()
        if at < len(up_copies):
            for entry in up_copies[at]:
                up_copy(*entry).start()

    up_stage(0)
    lax.fori_loop(1, 3, send_one, 0)

    loads[2].wait()
    loads[3].wait()

    def rs_copy(b):
        return pltpu.make_async_remote_copy(
            src_ref=rs_send.at[b], dst_ref=rs_recv.at[b],
            send_sem=rs_send_sem.at[b], recv_sem=rs_recv_sem.at[b],
            device_id={"ba": lax.rem(mb + b + 1, m)}, device_id_type=MESH,
        )

    def base(b, _):
        cols = pl.ds(pl.multiple_of(lax.rem(mb + b + 1, m) * kv, LANES), kv)
        rs_send[b, :, :kv] = jnp.dot(tok[...], kw[:, cols], preferred_element_type=F32)
        rs_send[b, :, kv:] = jnp.dot(tok[...], vw[:, cols], preferred_element_type=F32)

        @pl.when(b < m - 1)
        def _():
            rs_copy(b).start()

        return 0

    lax.fori_loop(0, m // 2, base, 0)
    up_stage(1)
    lax.fori_loop(3, 5, send_one, 0)
    lax.fori_loop(m // 2, m, base, 0)
    recv[0] = fill(0)
    up_stage(2)
    lax.fori_loop(5, n, send_one, 0)
    loads[4].wait()

    def add_part(b, _):
        rs_copy(b).wait_recv()
        rs_send[m - 1] += rs_recv[b]
        return 0

    width = resident * twice_rank
    slot_of_row = lax.broadcasted_iota(jnp.int32, (chunk, width), 0)
    column = lax.broadcasted_iota(jnp.int32, (chunk, width), 1)
    adapter_of_row = lax.rem(slot_of_row, quads) * groups + slot_of_row // stride
    own = adapter_of_row == column // twice_rank
    for_key = lax.rem(column, twice_rank) < rank

    def part_copy(b, i):
        return pltpu.make_async_remote_copy(
            src_ref=rank_part.at[i], dst_ref=rank_in.at[b, i],
            send_sem=p_send_sem.at[b, i], recv_sem=p_recv_sem.at[b, i],
            device_id={"ba": lax.rem(mb + b + 1, m)}, device_id_type=MESH,
        )

    def ret_copy(i):
        return pltpu.make_async_remote_copy(
            src_ref=ret_send.at[i], dst_ref=ret_recv.at[i],
            send_sem=r_send_sem.at[i], recv_sem=r_recv_sem.at[i],
            device_id={"aa": peer(i)}, device_id_type=MESH,
        )

    def partial(i):
        @pl.when(i > 0)
        def _():
            dispatch(i).wait_recv()

        wide = lax.dot_general(
            recv[i], down[...], (((1,), (1,)), ((), ())), preferred_element_type=F32
        )
        wide = jnp.where(own, wide, 0.0)
        total = wide[:, :LANES]
        for q in range(1, width // LANES):
            total = total + wide[:, q * LANES:(q + 1) * LANES]
        packed = total[:stride]
        for g in range(1, groups):
            packed = packed + total[g * stride:(g + 1) * stride]
        rank_part[i] = packed
        for b in range(m - 1):
            part_copy(b, i).start()

    def finish(i):
        total = rank_part[i]
        for b in range(m - 1):
            part_copy(b, i).wait_recv()
            total = total + rank_in[b, i]

        @pl.when(i == 0)
        def _():
            ret_recv[i] = total

        @pl.when(i > 0)
        def _():
            ret_send[i] = total
            ret_copy(i).start()

    def final(i):
        @pl.when(i > 0)
        def _():
            ret_copy(i).wait_recv()

        tall = jnp.concatenate([ret_recv[i]] * groups, axis=0)
        spread = jnp.where(own, jnp.concatenate([tall] * (width // LANES), axis=1), 0.0)
        key_hi, key_lo = split_two(jnp.where(for_key, spread, 0.0))
        value_hi, value_lo = split_two(jnp.where(for_key, 0.0, spread))
        bank = peer(i)
        up = up_all[bank]
        pieces = jnp.concatenate([key_hi, key_lo, value_hi, value_lo], axis=0)
        out = jnp.dot(pieces, up, preferred_element_type=F32)
        change = jnp.concatenate(
            [out[:chunk] + out[chunk:2 * chunk], out[2 * chunk:3 * chunk] + out[3 * chunk:]], axis=1
        )
        hi, lo = split_two(change)
        place = lax.broadcasted_iota(jnp.int32, (rows, chunk), 1) + bank * chunk
        pick = jnp.where(place == slot_col, 1.0, 0.0).astype(BF16)
        acc[...] += jnp.dot(pick, hi, preferred_element_type=F32) + jnp.dot(
            pick, lo, preferred_element_type=F32
        )

    def step(t, _):
        @pl.when((t >= 1) & (t < n + 1))
        def _():
            finish(t - 1)

        @pl.when(t == 2)
        def _():
            for at in range(3, len(up_copies) + 1):
                up_stage(at)
            lax.fori_loop(0, m - 1, add_part, 0)
            acc[...] = rs_send[m - 1]

        @pl.when(t >= 2)
        def _():
            final(t - 2)

        @pl.when(t < n)
        def _():
            partial(t)

        return 0

    lax.fori_loop(0, n + 2, step, 0)

    for stage in up_copies:
        for entry in stage:
            up_copy(*entry).wait_send()

    def drain(i, _):
        dispatch(i).wait_send()
        ret_copy(i).wait_send()
        return 0

    lax.fori_loop(1, n, drain, 0)

    def drain_parts(i, _):
        for b in range(m - 1):
            part_copy(b, i).wait_send()
        return 0

    lax.fori_loop(0, n, drain_parts, 0)
    for b in range(m - 1):
        rs_copy(b).wait_send()


def on_device(n, m, tokens, request_adapter_index, key_weight, value_weight, down_weight, up_weight):
    rows, width = tokens.shape
    resident, twice_rank, _ = down_weight.shape
    kv_width = key_weight.shape[1]
    kv = kv_width // m
    cap = max(2, 2 * rows // (resident * n))
    chunk = resident * cap
    packed = chunk * twice_rank // LANES
    flat = resident * twice_rank
    dma = pltpu.SemaphoreType.DMA
    total = pl.pallas_call(
        functools.partial(kernel, n, m, cap, resident, twice_rank),
        out_shape=jax.ShapeDtypeStruct((rows, 2 * kv), F32),
        in_specs=[pl.BlockSpec(memory_space=pltpu.VMEM)] + [pl.BlockSpec(memory_space=pl.ANY)] * 5,
        out_specs=pl.BlockSpec(memory_space=pltpu.VMEM),
        scratch_shapes=[
            pltpu.VMEM((rows, width), BF16),
            pltpu.VMEM((width, kv_width), BF16),
            pltpu.VMEM((width, kv_width), BF16),
            pltpu.VMEM((flat, width), BF16),
            pltpu.VMEM((n, flat, kv), BF16),
            pltpu.VMEM((n, chunk, width), BF16),
            pltpu.VMEM((n, chunk, width), BF16),
            pltpu.VMEM((m, rows, 2 * kv), F32),
            pltpu.VMEM((m - 1, rows, 2 * kv), F32),
            pltpu.VMEM((n, packed, LANES), F32),
            pltpu.VMEM((m - 1, n, packed, LANES), F32),
            pltpu.VMEM((n, packed, LANES), F32),
            pltpu.VMEM((n, packed, LANES), F32),
            dma((5,)),
            dma((n,)), dma((n,)), dma((n,)), dma((n,)),
            dma((m,)), dma((m,)),
            dma((m - 1, n)), dma((m - 1, n)),
            dma((n,)), dma((n,)),
        ],
        compiler_params=pltpu.CompilerParams(
            collective_id=0, has_side_effects=True, vmem_limit_bytes=56 * 1024 * 1024
        ),
    )(
        request_adapter_index.reshape(1, rows),
        tokens,
        key_weight,
        value_weight,
        down_weight.reshape(flat, width),
        up_weight.reshape(flat, kv_width),
    )
    return total[:, :kv].astype(BF16), total[:, kv:].astype(BF16)


def solution(mesh):
    return jax.shard_map(
        functools.partial(on_device, mesh.shape["aa"], mesh.shape["ba"]),
        mesh=mesh,
        in_specs=(
            P("aa", "ba"),
            P("aa", None),
            P("ba", None),
            P("ba", None),
            P("aa", None, "ba"),
            P("aa", None, None, None),
        ),
        out_specs=(P("aa", "ba"), P("aa", "ba")),
        check_vma=False,
    )
```
